32 devices in a mesh: seq: 8 (over z, y), head: 4 (over x, core).
Axes of the slice: x: 2, y: 2, z: 4, core: 2. Of those that a mesh axis runs over, the one named last changes fastest.
Arguments:
- queries: bfloat16 [4096, 8192], P(('seq', 'head')), may hold values from -8 to 8
- keys: bfloat16 [4096, 1024], P(('seq', 'head')), may hold values from -8 to 8
- values: bfloat16 [4096, 1024], P(('seq', 'head')), may hold values from -6 to 6
- selected: int32 [32, 8], P('seq'), may hold values from 0 to 31, as said below
- counts: int32 [32], P('seq'), may hold values from 1 to 8
- block_slot: int32 [32], P('seq'), may hold values from 0 to 31, as said below
Outputs:
- attended: bfloat16 [4096, 8192], P(('seq', 'head'))
The draws below stay inside these ranges and needn't reach their ends.
Inputs may be any that keep to these rules, and one draw needn't show every extreme that they name: A permutation of 0 to 31. Block b's rows of keys and values start at row 128 * block_slot[b]; its owner shard is block_slot[b] // 4. The 4 blocks of one sequence shard (blocks s * 4 onward) have distinct owner shards, and block_slot[b] % 4 == b % 4. `selected`: row q lists its live entries first: entry 0 is q itself, the other live entries are distinct blocks of earlier sequence shards; entries from counts[q] on are 0. Over the live entries of the 4 rows of one sequence shard, at most 2 distinct blocks have the same owner shard, and in every draw some shard reaches 2 from some owner.
All inputs are finite; a program needn't handle non-finite values.
Results may differ from the reference program's by a relative error of at most 0.0049.
Values may be sent and summed in bfloat16 or wider, within the bound.
A program may use at most 128 MiB of HBM per device.

```python
import math
import jax
import jax.numpy as jnp
from jax import lax

QUERY_HEADS = 64
KEY_VALUE_HEADS = 8
HEAD_SIZE = 128
BLOCK_ROWS = 128
SELECTION_COUNT = 8
BLK_SEQ = 4
NB = 32
TOKEN_COUNT = 4096
N_SEQ = 8


def selection_tables(key):
    base = jax.random.fold_in(key, 4049)
    keys_list = jax.random.split(base, 5)
    shard_perm = jax.random.permutation(keys_list[0], N_SEQ).astype(jnp.int32)
    offsets = jax.random.permutation(keys_list[1], N_SEQ)[:BLK_SEQ].astype(jnp.int32)
    blocks = jnp.arange(NB, dtype=jnp.int32)
    home_shard = blocks // BLK_SEQ
    within = blocks % BLK_SEQ
    owner_of = (shard_perm[home_shard] + offsets[within]) % N_SEQ
    slot_of = owner_of * BLK_SEQ + within
    by_slot = jnp.zeros((NB,), jnp.int32).at[slot_of].set(blocks)
    slot_grid = by_slot.reshape(N_SEQ, BLK_SEQ)
    grid_shard = slot_grid // BLK_SEQ
    rank_draw = jax.random.randint(keys_list[2], (N_SEQ, N_SEQ, BLK_SEQ), 0, 1 << 20) * BLK_SEQ + jnp.arange(BLK_SEQ, dtype=jnp.int32)
    requesters = jnp.arange(N_SEQ, dtype=jnp.int32)[:, None, None]
    masked = jnp.where(grid_shard[None] < requesters, rank_draw, -1)
    best_pick = jnp.argmax(masked, axis=2).astype(jnp.int32)
    extra_ok = jnp.max(masked, axis=2) >= 0
    spread_grid = jnp.broadcast_to(slot_grid[None], (N_SEQ, N_SEQ, BLK_SEQ))
    extra_block = jnp.take_along_axis(spread_grid, best_pick[:, :, None], axis=2)[:, :, 0]
    priority = jax.random.randint(keys_list[3], (NB, N_SEQ), 0, 1 << 20) * N_SEQ + jnp.arange(N_SEQ, dtype=jnp.int32)[None, :]
    first_owner = owner_of[home_shard * BLK_SEQ]
    forced = (within == BLK_SEQ - 1)[:, None] & (jnp.arange(N_SEQ, dtype=jnp.int32)[None, :] == first_owner[:, None])
    priority = jnp.where(forced, 1 << 30, priority)
    usable = extra_ok[home_shard]
    priority = jnp.where(usable, priority, -1)
    top_values, top_index = lax.top_k(priority, SELECTION_COUNT - 1)
    picked = jnp.take_along_axis(extra_block[home_shard], top_index, axis=1)
    pool_size = jnp.sum(usable.astype(jnp.int32), axis=1)
    want_count = jax.random.randint(keys_list[4], (NB,), SELECTION_COUNT // 2, SELECTION_COUNT)
    extra_count = jnp.minimum(want_count, pool_size).astype(jnp.int32)
    position = jnp.arange(SELECTION_COUNT - 1, dtype=jnp.int32)[None, :]
    picked = jnp.where(position < extra_count[:, None], picked, 0).astype(jnp.int32)
    chosen = jnp.concatenate([blocks[:, None], picked], axis=1).astype(jnp.int32)
    return (slot_of.astype(jnp.int32), chosen, (1 + extra_count).astype(jnp.int32))


def draw_selected(key, part):
    return selection_tables(key)[1]


def draw_counts(key, part):
    return selection_tables(key)[2]


def draw_block_slot(key, part):
    return selection_tables(key)[0]


def draw_queries(key, part):
    random_portion = jax.random.normal(jax.random.fold_in(key, 11), (TOKEN_COUNT, QUERY_HEADS, HEAD_SIZE), jnp.float32)
    sampled_blocks = random_portion
    return jnp.clip(sampled_blocks, -8.0, 8.0).reshape(TOKEN_COUNT, QUERY_HEADS * HEAD_SIZE).astype(jnp.bfloat16)


def draw_keys(key, part):
    random_portion = jax.random.normal(jax.random.fold_in(key, 21), (TOKEN_COUNT, KEY_VALUE_HEADS, HEAD_SIZE), jnp.float32)
    sampled_blocks = random_portion
    return jnp.clip(sampled_blocks, -8.0, 8.0).reshape(TOKEN_COUNT, KEY_VALUE_HEADS * HEAD_SIZE).astype(jnp.bfloat16)


def shard_levels(stream_key, dims, pieces, least, largest):
    def one(dim, shards_of):
        heights = jax.random.uniform(jax.random.fold_in(jax.random.fold_in(stream_key, 6), dim), (shards_of,), jnp.float32, least / len(pieces), largest / len(pieces))
        return jnp.repeat(jnp.exp(heights), dims[dim] // shards_of).reshape((-1,) + (1,) * (len(dims) - dim - 1))

    level = one(*pieces[0])
    for cut in pieces[1:]:
        level = level * one(*cut)
    return level


def centred(key, dims, width, limit, cuts=(), kind=jnp.bfloat16):
    gain = shard_levels(key, dims, cuts, -0.22, 0.18) if cuts else 1.0
    entries = jax.random.normal(key, dims, jnp.float32) * width * gain
    return jnp.minimum(jnp.maximum(entries, -limit), limit).astype(kind)


def setup_inputs(seed: int = 0) -> dict:
    splits = jax.random.split(jax.random.key(seed), 7)
    queries = draw_queries(jax.random.fold_in(splits[6], 71), 0)
    keys = draw_keys(jax.random.fold_in(splits[6], 71), 0)
    values = centred(splits[2], (TOKEN_COUNT, KEY_VALUE_HEADS * HEAD_SIZE), 1.0, 6.0, ((0, 32),))
    selected = draw_selected(jax.random.fold_in(splits[6], 71), 0)
    counts = draw_counts(jax.random.fold_in(splits[6], 71), 0)
    block_slot = draw_block_slot(jax.random.fold_in(splits[6], 71), 0)
    return dict(queries=queries, keys=keys, values=values, selected=selected, counts=counts, block_slot=block_slot)


def reference(queries, keys, values, selected, counts, block_slot):
    block_count = selected.shape[0]
    heads_per_group = QUERY_HEADS // KEY_VALUE_HEADS
    score_scale = 1.0 / math.sqrt(HEAD_SIZE)
    key_block_list = keys.reshape(block_count, BLOCK_ROWS, KEY_VALUE_HEADS, HEAD_SIZE)
    value_block_list = values.reshape(block_count, BLOCK_ROWS, KEY_VALUE_HEADS, HEAD_SIZE)
    query_block_list = queries.reshape(block_count, BLOCK_ROWS, KEY_VALUE_HEADS, heads_per_group, HEAD_SIZE)

    def one_block(operands):
        block_id, query_tile, chosen, live_count = operands
        holder_shard = block_slot[chosen]
        key_block_rows = key_block_list[holder_shard].reshape(SELECTION_COUNT * BLOCK_ROWS, KEY_VALUE_HEADS, HEAD_SIZE)
        value_block_rows = value_block_list[holder_shard].reshape(SELECTION_COUNT * BLOCK_ROWS, KEY_VALUE_HEADS, HEAD_SIZE)
        scores = jnp.einsum('igmd,kgd->gmik', query_tile.astype(jnp.float32), key_block_rows.astype(jnp.float32)) * score_scale
        query_pos = block_id * BLOCK_ROWS + jnp.arange(BLOCK_ROWS, dtype=jnp.int32)
        key_pos = (chosen[:, None] * BLOCK_ROWS + jnp.arange(BLOCK_ROWS, dtype=jnp.int32)[None, :]).reshape(-1)
        live_entry = jnp.repeat(jnp.arange(SELECTION_COUNT, dtype=jnp.int32) < live_count, BLOCK_ROWS)
        visible = live_entry[None, :] & (key_pos[None, :] <= query_pos[:, None])
        scores = jnp.where(visible[None, None], scores, -jnp.inf)
        row_top = lax.optimization_barrier(jnp.max(scores, axis=-1, keepdims=True))
        weights = jnp.exp(scores - row_top)
        probability = (weights / lax.optimization_barrier(jnp.sum(weights, axis=-1, keepdims=True))).astype(jnp.bfloat16)
        mixed_out = jnp.einsum('gmik,kgd->igmd', probability.astype(jnp.float32), value_block_rows.astype(jnp.float32))
        return mixed_out.astype(jnp.bfloat16).reshape(BLOCK_ROWS, QUERY_HEADS * HEAD_SIZE)
    attended = lax.map(one_block, (jnp.arange(block_count, dtype=jnp.int32), query_block_list, selected, counts))
    return attended.reshape(block_count * BLOCK_ROWS, QUERY_HEADS * HEAD_SIZE)
```

```python
import functools
import math

import jax
import jax.numpy as jnp
from jax import lax
from jax.experimental import pallas as pl
from jax.experimental.pallas import tpu as pltpu
from jax.sharding import PartitionSpec as P

QUERY_HEADS = 64
KEY_VALUE_HEADS = 8
HEAD_SIZE = 128
BLOCK_ROWS = 128
MESH = pl.DeviceIdType.MESH


def kernel(ns, nh, groups, entries, q_ref, k_ref, v_ref, sel_ref, cnt_ref, slot_ref, out_ref,
           qbuf, obuf, kcat, vcat, diag, slots_v, slots_s,
           hs, hr, qs, qr, us, ur, ds_, dr, ys, yr, os_, or_, ss, sr, slot_sem, *kv):
    s = lax.axis_index("seq")
    h = lax.axis_index("head")
    ysz = 2 if ns % 2 == 0 else 1
    zsz = ns // ysz
    z = s // ysz
    y = s % ysz
    y_peer = s + 1 - 2 * y
    width = qbuf.shape[3]
    heads_per_group = width // HEAD_SIZE
    rotation = [nh // 2] + [d for d in range(nh - 1, 0, -1) if d != nh // 2]

    def remote(src, dst, send, recv, dev):
        return pltpu.make_async_remote_copy(
            src_ref=src, dst_ref=dst, send_sem=send, recv_sem=recv,
            device_id=dev, device_id_type=MESH)

    barrier = pltpu.get_barrier_semaphore()
    for d in range(1, nh):
        pl.semaphore_signal(barrier, inc=1, device_id=(s, (h + d) % nh), device_id_type=MESH)
    for d in range(1, ns):
        pl.semaphore_signal(barrier, inc=1, device_id=((s + d) % ns, h), device_id_type=MESH)
    pl.semaphore_wait(barrier, nh - 1 + ns - 1)

    def lanes(unit, size):
        return pl.ds(pl.multiple_of(unit * size, size), size)

    def kv_head(g, t, d):
        peer = (h + d) % nh
        src = (k_ref, v_ref)[t]
        return remote(src.at[:, lanes(peer * groups + g, HEAD_SIZE)], kv[g].at[s * nh + h, t],
                      hs.at[g, t, d - 1], hr.at[g, t, d - 1], (s, peer))

    def kv_head_in(g, t, d):
        peer = (h + nh - d) % nh
        src = (k_ref, v_ref)[t]
        return remote(src.at[:, lanes(peer * groups + g, HEAD_SIZE)], kv[g].at[s * nh + peer, t],
                      hs.at[g, t, d - 1], hr.at[g, t, d - 1], (s, peer))

    def q_head(g, d):
        peer = (h + d) % nh
        return remote(q_ref.at[:, lanes(peer * groups + g, width)], qbuf.at[g, h],
                      qs.at[g, d - 1], qr.at[g, d - 1], (s, peer))

    def q_head_in(g, d):
        peer = (h + nh - d) % nh
        return remote(q_ref.at[:, lanes(peer * groups + g, width)], qbuf.at[g, peer],
                      qs.at[g, d - 1], qr.at[g, d - 1], (s, peer))

    def slot_out(d):
        return remote(slot_ref, slots_v.at[s], ss.at[d - 1], sr.at[d - 1], ((s + d) % ns, h))

    def slot_in(d):
        peer = (s + ns - d) % ns
        return remote(slot_ref, slots_v.at[peer], ss.at[d - 1], sr.at[d - 1], (peer, h))

    for g in range(groups):
        for d in rotation:
            for t in range(2):
                kv_head(g, t, d).start()
    for d in range(1, ns):
        slot_out(d).start()
    for g in range(groups):
        for d in rotation:
            q_head(g, d).start()

    for g in range(groups):
        kv[g][s * nh + h, 0] = k_ref[:, lanes(h * groups + g, HEAD_SIZE)]
        kv[g][s * nh + h, 1] = v_ref[:, lanes(h * groups + g, HEAD_SIZE)]
        qbuf[g, h] = q_ref[:, lanes(h * groups + g, width)]
    slots_v[s] = slot_ref[...]
    pair_rows = 2 * BLOCK_ROWS
    row = lax.rem(lax.broadcasted_iota(jnp.int32, (pair_rows, BLOCK_ROWS), 0), BLOCK_ROWS)
    col = lax.broadcasted_iota(jnp.int32, (pair_rows, BLOCK_ROWS), 1)
    diag[...] = jnp.where(col <= row, 0.0, -jnp.inf).astype(jnp.float32)
    vcat[:, HEAD_SIZE:] = jnp.ones((entries * BLOCK_ROWS, HEAD_SIZE), jnp.bfloat16)

    def chunk(g, shard):
        return kv[g].at[pl.ds(shard * nh, nh)]

    def up(g, t, shard, dev):
        return remote(chunk(g, shard), chunk(g, shard), us.at[g, t], ur.at[g, t], (dev, h))

    def down(g, t, shard, dev):
        return remote(chunk(g, shard), chunk(g, shard), ds_.at[g, t], dr.at[g, t], (dev, h))

    def across(g, i, shard):
        return remote(chunk(g, shard), chunk(g, shard), ys.at[g, i], yr.at[g, i], (y_peer, h))

    def gather_start(g):
        for d in rotation:
            for t in range(2):
                kv_head_in(g, t, d).wait_recv()
        if ysz > 1:
            across(g, 0, s).start()
        if zsz > 1:
            @pl.when(z < zsz - 1)
            def _():
                up(g, 0, s, s + ysz).start()

            @pl.when(z > 0)
            def _():
                down(g, 0, s, s - ysz).start()

    def gather_step(g, t):
        below = s - (1 + t) * ysz
        above = s + (1 + t) * ysz

        @pl.when(z - 1 - t >= 0)
        def _():
            up(g, t, below, s).wait_recv()
            if t + 1 < zsz - 1:
                @pl.when(z < zsz - 1)
                def _():
                    up(g, t + 1, below, s + ysz).start()
            if ysz > 1:
                across(g, 1 + t, below).start()

        @pl.when(z + 1 + t <= zsz - 1)
        def _():
            down(g, t, above, s).wait_recv()
            if t + 1 < zsz - 1:
                @pl.when(z > 0)
                def _():
                    down(g, t + 1, above, s - ysz).start()
            if ysz > 1:
                across(g, zsz + t, above).start()

    def gather_end(g):
        if ysz > 1:
            across(g, 0, y_peer).wait_recv()
            for t in range(zsz - 1):
                @pl.when(z - 1 - t >= 0)
                def _():
                    across(g, 1 + t, y_peer - (1 + t) * ysz).wait_recv()

                @pl.when(z + 1 + t <= zsz - 1)
                def _():
                    across(g, zsz + t, y_peer + (1 + t) * ysz).wait_recv()

    def gather_drain(g):
        if ysz > 1:
            across(g, 0, s).wait_send()
        for t in range(zsz - 1):
            @pl.when((z < zsz - 1) & (z - t >= 0))
            def _():
                up(g, t, s - t * ysz, s + ysz).wait_send()

            @pl.when((z > 0) & (z + t <= zsz - 1))
            def _():
                down(g, t, s + t * ysz, s - ysz).wait_send()
            if ysz > 1:
                @pl.when(z - 1 - t >= 0)
                def _():
                    across(g, 1 + t, s - (1 + t) * ysz).wait_send()

                @pl.when(z + 1 + t <= zsz - 1)
                def _():
                    across(g, zsz + t, s + (1 + t) * ysz).wait_send()

    factor = math.log2(math.e) / math.sqrt(HEAD_SIZE)
    blk_seq = sel_ref.shape[0]

    def fetch(g, j):
        for e in range(entries):
            b = sel_ref[j, e]
            place = slots_s[lax.div(b, blk_seq), 0, lax.rem(b, blk_seq)]
            rows = slice(e * BLOCK_ROWS, (e + 1) * BLOCK_ROWS)
            kcat[rows, :] = kv[g][place, 0]
            vcat[rows, :HEAD_SIZE] = kv[g][place, 1]

    def attend(g, j):
        rest = lax.broadcasted_iota(jnp.int32, (1, (entries - 1) * BLOCK_ROWS), 1) + BLOCK_ROWS
        bias = jnp.where(rest < cnt_ref[j] * BLOCK_ROWS, 0.0, -jnp.inf).astype(jnp.float32)

        def pair(i, _):
            cols = pl.multiple_of(i * 2 * HEAD_SIZE, 2 * HEAD_SIZE)
            q2 = qbuf[g, j, :, pl.ds(cols, 2 * HEAD_SIZE)]
            q2 = jnp.concatenate([q2[:, :HEAD_SIZE], q2[:, HEAD_SIZE:]], axis=0)
            scores = lax.dot_general(q2, kcat[...], (((1,), (1,)), ((), ())),
                                     preferred_element_type=jnp.float32)
            own = scores[:, :BLOCK_ROWS] + diag[...]
            others = scores[:, BLOCK_ROWS:] + bias
            scores = jnp.concatenate([own, others], axis=1)
            top = jnp.max(scores, axis=1, keepdims=True)
            weights = jnp.exp2((scores - top) * factor).astype(jnp.bfloat16)
            mixed = jnp.dot(weights, vcat[...], preferred_element_type=jnp.float32)
            result = (mixed[:, :HEAD_SIZE] / mixed[:, HEAD_SIZE:]).astype(jnp.bfloat16)
            obuf[g, j, :, pl.ds(cols, HEAD_SIZE)] = result[:BLOCK_ROWS]
            obuf[g, j, :, pl.ds(cols + HEAD_SIZE, HEAD_SIZE)] = result[BLOCK_ROWS:]
            return 0

        lax.fori_loop(0, heads_per_group // 2, pair, 0)

    def result_out(g, d):
        peer = (h + d) % nh
        return remote(obuf.at[g, peer], out_ref.at[:, lanes(h * groups + g, width)],
                      os_.at[g, d - 1], or_.at[g, d - 1], (s, peer))

    def result_in(g, d):
        peer = (h + nh - d) % nh
        return remote(obuf.at[g, peer], out_ref.at[:, lanes(peer * groups + g, width)],
                      os_.at[g, d - 1], or_.at[g, d - 1], (s, peer))

    gather_start(0)
    for t in range(zsz - 1):
        gather_step(0, t)
    for d in range(1, ns):
        slot_in(d).wait_recv()
    slot_copy = pltpu.make_async_copy(slots_v, slots_s, slot_sem)
    slot_copy.start()
    slot_copy.wait()

    order = rotation + [0]
    pending = None
    for g in range(groups):
        steps = []
        if g + 1 < groups:
            gather_start(g + 1)
            steps = list(range(zsz - 1))
            if steps:
                gather_step(g + 1, steps.pop(0))
        gather_end(g)
        for d in order:
            j = (h + d) % nh
            fetch(g, j)
            if pending is not None:
                result_out(*pending).start()
                pending = None
            if d:
                q_head_in(g, nh - d).wait_recv()
            attend(g, j)
            if d:
                pending = (g, d)
            else:
                out_ref[:, lanes(h * groups + g, width)] = obuf[g, h]
            if steps:
                gather_step(g + 1, steps.pop(0))
        for t in steps:
            gather_step(g + 1, t)

    for g in range(groups):
        gather_drain(g)
        for d in rotation:
            for t in range(2):
                kv_head(g, t, d).wait_send()
            q_head(g, d).wait_send()
    for d in range(1, ns):
        slot_out(d).wait_send()
    for g in range(groups):
        for d in rotation:
            result_out(g, d).wait_send()
            result_in(g, d).wait_recv()


def body(queries, keys, values, selected, counts, block_slot):
    ns = lax.axis_size("seq")
    nh = lax.axis_size("head")
    blk_seq, entries = selected.shape
    rows = queries.shape[0]
    groups = keys.shape[1] // HEAD_SIZE // nh
    width = queries.shape[1] // nh // groups
    assert rows == BLOCK_ROWS and blk_seq == nh
    slots = jnp.pad(block_slot, (0, 128 - blk_seq)).reshape(1, 128)
    vmem = pl.BlockSpec(memory_space=pltpu.VMEM)
    smem = pl.BlockSpec(memory_space=pltpu.SMEM)
    zsz = ns // (2 if ns % 2 == 0 else 1)
    dma = pltpu.SemaphoreType.DMA
    steps = max(zsz - 1, 1)
    return pl.pallas_call(
        functools.partial(kernel, ns, nh, groups, entries),
        out_shape=jax.ShapeDtypeStruct(queries.shape, jnp.bfloat16),
        in_specs=[vmem, vmem, vmem, smem, smem, vmem],
        out_specs=vmem,
        scratch_shapes=[
            pltpu.VMEM((groups, nh, rows, width), jnp.bfloat16),
            pltpu.VMEM((groups, nh, rows, width), jnp.bfloat16),
            pltpu.VMEM((entries * BLOCK_ROWS, HEAD_SIZE), jnp.bfloat16),
            pltpu.VMEM((entries * BLOCK_ROWS, 2 * HEAD_SIZE), jnp.bfloat16),
            pltpu.VMEM((2 * BLOCK_ROWS, BLOCK_ROWS), jnp.float32),
            pltpu.VMEM((ns, 1, 128), jnp.int32),
            pltpu.SMEM((ns, 1, 128), jnp.int32),
            dma((groups, 2, nh - 1)), dma((groups, 2, nh - 1)),
            dma((groups, nh - 1)), dma((groups, nh - 1)),
            dma((groups, steps)), dma((groups, steps)),
            dma((groups, steps)), dma((groups, steps)),
            dma((groups, 2 * zsz)), dma((groups, 2 * zsz)),
            dma((groups, nh - 1)), dma((groups, nh - 1)),
            dma((ns - 1,)), dma((ns - 1,)),
            dma,
        ] + [pltpu.VMEM((ns * nh, 2, BLOCK_ROWS, HEAD_SIZE), jnp.bfloat16)] * groups,
        compiler_params=pltpu.CompilerParams(
            collective_id=0, has_side_effects=True, vmem_limit_bytes=60 * 1024 * 1024),
        name="block_attention",
    )(queries, keys, values, selected, counts, slots)


def solution(mesh):
    return jax.shard_map(
        body,
        mesh=mesh,
        in_specs=(
            P(("seq", "head"), None),
            P(("seq", "head"), None),
            P(("seq", "head"), None),
            P("seq", None),
            P("seq"),
            P("seq"),
        ),
        out_specs=P(("seq", "head"), None),
        check_vma=False,
    )
```

```python
import functools
import math

import jax
import jax.numpy as jnp
from jax import lax
from jax.experimental import pallas as pl
from jax.experimental.pallas import tpu as pltpu
from jax.sharding import PartitionSpec as P

QUERY_HEADS = 64
KEY_VALUE_HEADS = 8
HEAD_SIZE = 128
BLOCK_ROWS = 128
MESH = pl.DeviceIdType.MESH


def kernel(ns, nh, groups, entries, q_ref, k_ref, v_ref, sel_ref, cnt_ref, own_slot_ref, out_ref,
           qbuf, obuf, kcat, vcat, diag, slot_ref, slots_v, slots_s,
           hs, hr, qs, qr, us, ur, ds_, dr, ys, yr, os_, or_, ss, sr, slot_sem, *kv):
    s = lax.axis_index("seq")
    h = lax.axis_index("head")
    ysz = 2 if ns % 2 == 0 else 1
    zsz = ns // ysz
    z = s // ysz
    y = s % ysz
    y_peer = s + 1 - 2 * y
    width = qbuf.shape[3]
    heads_per_group = width // HEAD_SIZE
    rotation = [nh // 2] + [d for d in range(nh - 1, 0, -1) if d != nh // 2]

    def remote(src, dst, send, recv, dev):
        return pltpu.make_async_remote_copy(
            src_ref=src, dst_ref=dst, send_sem=send, recv_sem=recv,
            device_id=dev, device_id_type=MESH)

    lane = lax.broadcasted_iota(jnp.int32, (1, 128), 1)
    slot_row = jnp.zeros((1, 128), jnp.int32)
    for i in range(sel_ref.shape[0]):
        slot_row = jnp.where(lane == i, own_slot_ref[i], slot_row)
    slot_ref[...] = slot_row

    barrier = pltpu.get_barrier_semaphore()
    for d in range(1, nh):
        pl.semaphore_signal(barrier, inc=1, device_id=(s, (h + d) % nh), device_id_type=MESH)
    for d in range(1, ns):
        pl.semaphore_signal(barrier, inc=1, device_id=((s + d) % ns, h), device_id_type=MESH)
    pl.semaphore_wait(barrier, nh - 1 + ns - 1)

    def lanes(unit, size):
        return pl.ds(pl.multiple_of(unit * size, size), size)

    def kv_head(g, t, d):
        peer = (h + d) % nh
        src = (k_ref, v_ref)[t]
        return remote(src.at[:, lanes(peer * groups + g, HEAD_SIZE)], kv[g].at[s * nh + h, t],
                      hs.at[g, t, d - 1], hr.at[g, t, d - 1], (s, peer))

    def kv_head_in(g, t, d):
        peer = (h + nh - d) % nh
        src = (k_ref, v_ref)[t]
        return remote(src.at[:, lanes(peer * groups + g, HEAD_SIZE)], kv[g].at[s * nh + peer, t],
                      hs.at[g, t, d - 1], hr.at[g, t, d - 1], (s, peer))

    def q_head(g, d):
        peer = (h + d) % nh
        return remote(q_ref.at[:, lanes(peer * groups + g, width)], qbuf.at[g, h],
                      qs.at[g, d - 1], qr.at[g, d - 1], (s, peer))

    def q_head_in(g, d):
        peer = (h + nh - d) % nh
        return remote(q_ref.at[:, lanes(peer * groups + g, width)], qbuf.at[g, peer],
                      qs.at[g, d - 1], qr.at[g, d - 1], (s, peer))

    def slot_out(d):
        return remote(slot_ref, slots_v.at[s], ss.at[d - 1], sr.at[d - 1], ((s + d) % ns, h))

    def slot_in(d):
        peer = (s + ns - d) % ns
        return remote(slot_ref, slots_v.at[peer], ss.at[d - 1], sr.at[d - 1], (peer, h))

    for g in range(groups):
        for d in rotation:
            for t in range(2):
                kv_head(g, t, d).start()
    for d in range(1, ns):
        slot_out(d).start()
    for g in range(groups):
        for d in rotation:
            q_head(g, d).start()

    for g in range(groups):
        kv[g][s * nh + h, 0] = k_ref[:, lanes(h * groups + g, HEAD_SIZE)]
        kv[g][s * nh + h, 1] = v_ref[:, lanes(h * groups + g, HEAD_SIZE)]
        qbuf[g, h] = q_ref[:, lanes(h * groups + g, width)]
    slots_v[s] = slot_ref[...]
    pair_rows = 2 * BLOCK_ROWS
    row = lax.rem(lax.broadcasted_iota(jnp.int32, (pair_rows, BLOCK_ROWS), 0), BLOCK_ROWS)
    col = lax.broadcasted_iota(jnp.int32, (pair_rows, BLOCK_ROWS), 1)
    diag[...] = jnp.where(col <= row, 0.0, -jnp.inf).astype(jnp.float32)
    vcat[:, HEAD_SIZE:] = jnp.ones((entries * BLOCK_ROWS, HEAD_SIZE), jnp.bfloat16)

    half = nh // 2

    def early(g):
        return ysz > 1 and nh > 2 and g == groups - 1

    def part(g, shard, piece):
        lo, size = ((0, half), (half, nh - half), (nh - 1, 1))[piece]
        return kv[g].at[pl.ds(shard * nh + lo, size)]

    def cross_part(g, shard, piece):
        if piece == 1 and early(g):
            return kv[g].at[pl.ds(shard * nh + half, nh - 1 - half)]
        return part(g, shard, piece)

    def up(g, p, t, shard, dev):
        ref = part(g, shard, p)
        return remote(ref, ref, us.at[g, p, t], ur.at[g, p, t], (dev, h))

    def down(g, p, t, shard, dev):
        ref = part(g, shard, p)
        return remote(ref, ref, ds_.at[g, p, t], dr.at[g, p, t], (dev, h))

    def across(g, p, i, shard):
        ref = cross_part(g, shard, p)
        return remote(ref, ref, ys.at[g, p, i], yr.at[g, p, i], (y_peer, h))

    def pieces(g):
        return (0, 1, 2) if early(g) else (0, 1)

    def column(p):
        return y_peer if p == 2 else s

    def send_both(g, p):
        if zsz > 1:
            @pl.when(z < zsz - 1)
            def _():
                up(g, p, 0, column(p), s + ysz).start()

            @pl.when(z > 0)
            def _():
                down(g, p, 0, column(p), s - ysz).start()

    def gather_z(g):
        for d in rotation:
            for t in range(2):
                kv_head_in(g, t, d).wait_recv()
        if early(g):
            across(g, 2, 0, s).start()
        send_both(g, 0)
        send_both(g, 1)

    def gather_y(g):
        if ysz > 1:
            across(g, 0, 0, s).start()
            across(g, 1, 0, s).start()
        if early(g):
            across(g, 2, 0, y_peer).wait_recv()
            send_both(g, 2)

    def gather_step(g, t):
        for p in pieces(g):
            below = column(p) - (1 + t) * ysz
            above = column(p) + (1 + t) * ysz

            @pl.when(z - 1 - t >= 0)
            def _():
                up(g, p, t, below, s).wait_recv()
                if t + 1 < zsz - 1:
                    @pl.when(z < zsz - 1)
                    def _():
                        up(g, p, t + 1, below, s + ysz).start()
                if ysz > 1 and p < 2:
                    across(g, p, 1 + t, below).start()

            @pl.when(z + 1 + t <= zsz - 1)
            def _():
                down(g, p, t, above, s).wait_recv()
                if t + 1 < zsz - 1:
                    @pl.when(z > 0)
                    def _():
                        down(g, p, t + 1, above, s - ysz).start()
                if ysz > 1 and p < 2:
                    across(g, p, zsz + t, above).start()

    def gather_end(g):
        if ysz > 1:
            for p in range(2):
                across(g, p, 0, y_peer).wait_recv()
            for t in range(zsz - 1):
                for p in range(2):
                    @pl.when(z - 1 - t >= 0)
                    def _():
                        across(g, p, 1 + t, y_peer - (1 + t) * ysz).wait_recv()

                    @pl.when(z + 1 + t <= zsz - 1)
                    def _():
                        across(g, p, zsz + t, y_peer + (1 + t) * ysz).wait_recv()

    def gather_drain(g):
        for p in pieces(g):
            if ysz > 1:
                across(g, p, 0, s).wait_send()
            for t in range(zsz - 1):
                @pl.when((z < zsz - 1) & (z - t >= 0))
                def _():
                    up(g, p, t, column(p) - t * ysz, s + ysz).wait_send()

                @pl.when((z > 0) & (z + t <= zsz - 1))
                def _():
                    down(g, p, t, column(p) + t * ysz, s - ysz).wait_send()
                if ysz > 1 and p < 2:
                    @pl.when(z - 1 - t >= 0)
                    def _():
                        across(g, p, 1 + t, s - (1 + t) * ysz).wait_send()

                    @pl.when(z + 1 + t <= zsz - 1)
                    def _():
                        across(g, p, zsz + t, s + (1 + t) * ysz).wait_send()

    factor = math.log2(math.e) / math.sqrt(HEAD_SIZE)
    blk_seq = sel_ref.shape[0]

    def fetch(g, j):
        for e in range(entries):
            b = sel_ref[j, e]
            place = slots_s[lax.div(b, blk_seq), 0, lax.rem(b, blk_seq)]
            rows = slice(e * BLOCK_ROWS, (e + 1) * BLOCK_ROWS)
            kcat[rows, :] = kv[g][place, 0]
            vcat[rows, :HEAD_SIZE] = kv[g][place, 1]

    def attend(g, j):
        rest = lax.broadcasted_iota(jnp.int32, (1, (entries - 1) * BLOCK_ROWS), 1) + BLOCK_ROWS
        bias = jnp.where(rest < cnt_ref[j] * BLOCK_ROWS, 0.0, -jnp.inf).astype(jnp.float32)

        def pair(i, _):
            cols = pl.multiple_of(i * 2 * HEAD_SIZE, 2 * HEAD_SIZE)
            q2 = qbuf[g, j, :, pl.ds(cols, 2 * HEAD_SIZE)]
            q2 = jnp.concatenate([q2[:, :HEAD_SIZE], q2[:, HEAD_SIZE:]], axis=0)
            scores = lax.dot_general(q2, kcat[...], (((1,), (1,)), ((), ())),
                                     preferred_element_type=jnp.float32)
            own = scores[:, :BLOCK_ROWS] + diag[...]
            others = scores[:, BLOCK_ROWS:] + bias
            scores = jnp.concatenate([own, others], axis=1)
            top = jnp.max(scores, axis=1, keepdims=True)
            weights = jnp.exp2((scores - top) * factor).astype(jnp.bfloat16)
            mixed = jnp.dot(weights, vcat[...], preferred_element_type=jnp.float32)
            result = (mixed[:, :HEAD_SIZE] / mixed[:, HEAD_SIZE:]).astype(jnp.bfloat16)
            obuf[g, j, :, pl.ds(cols, HEAD_SIZE)] = result[:BLOCK_ROWS]
            obuf[g, j, :, pl.ds(cols + HEAD_SIZE, HEAD_SIZE)] = result[BLOCK_ROWS:]
            return 0

        lax.fori_loop(0, heads_per_group // 2, pair, 0, unroll=True)

    def result_out(g, d):
        peer = (h + d) % nh
        return remote(obuf.at[g, peer], out_ref.at[:, lanes(h * groups + g, width)],
                      os_.at[g, d - 1], or_.at[g, d - 1], (s, peer))

    def result_in(g, d):
        peer = (h + nh - d) % nh
        return remote(obuf.at[g, peer], out_ref.at[:, lanes(peer * groups + g, width)],
                      os_.at[g, d - 1], or_.at[g, d - 1], (s, peer))

    def slot_table():
        for d in range(1, ns):
            slot_in(d).wait_recv()
        slot_copy = pltpu.make_async_copy(slots_v, slots_s, slot_sem)
        slot_copy.start()
        slot_copy.wait()

    if nh == 4:
        order = [2, 3 - 2 * (h % 2), 1 + 2 * (h % 2), 0]
    else:
        order = rotation + [0]
    gather_z(0)
    gather_y(0)
    for t in range(zsz - 2):
        gather_step(0, t)
    pending = None
    for g in range(groups):
        more = g + 1 < groups
        if more:
            gather_z(g + 1)
        if g == 0 and zsz > 1:
            gather_step(0, zsz - 2)
        steps = []
        if more:
            gather_y(g + 1)
            steps = list(range(zsz - 1))
            if steps:
                gather_step(g + 1, steps.pop(0))
        if g == 0:
            slot_table()
        gather_end(g)
        for n, d in enumerate(order):
            own = n == len(order) - 1
            j = (h + d) % nh
            fetch(g, j)
            if pending is not None:
                result_out(*pending).start()
                pending = None
            if not own:
                q_head_in(g, nh - d).wait_recv()
            attend(g, j)
            if own:
                out_ref[:, lanes(h * groups + g, width)] = obuf[g, h]
            else:
                pending = (g, d)
            if steps:
                gather_step(g + 1, steps.pop(0))
        for t in steps:
            gather_step(g + 1, t)

    for g in range(groups):
        gather_drain(g)
        for d in rotation:
            for t in range(2):
                kv_head(g, t, d).wait_send()
            q_head(g, d).wait_send()
    for d in range(1, ns):
        slot_out(d).wait_send()
    for g in range(groups):
        for d in rotation:
            result_out(g, d).wait_send()
            result_in(g, d).wait_recv()


def body(queries, keys, values, selected, counts, block_slot):
    ns = lax.axis_size("seq")
    nh = lax.axis_size("head")
    blk_seq, entries = selected.shape
    rows = queries.shape[0]
    groups = keys.shape[1] // HEAD_SIZE // nh
    width = queries.shape[1] // nh // groups
    assert rows == BLOCK_ROWS and blk_seq == nh
    vmem = pl.BlockSpec(memory_space=pltpu.VMEM)
    smem = pl.BlockSpec(memory_space=pltpu.SMEM)
    zsz = ns // (2 if ns % 2 == 0 else 1)
    dma = pltpu.SemaphoreType.DMA
    steps = max(zsz - 1, 1)
    return pl.pallas_call(
        functools.partial(kernel, ns, nh, groups, entries),
        out_shape=jax.ShapeDtypeStruct(queries.shape, jnp.bfloat16),
        in_specs=[vmem, vmem, vmem, smem, smem, smem],
        out_specs=vmem,
        scratch_shapes=[
            pltpu.VMEM((groups, nh, rows, width), jnp.bfloat16),
            pltpu.VMEM((groups, nh, rows, width), jnp.bfloat16),
            pltpu.VMEM((entries * BLOCK_ROWS, HEAD_SIZE), jnp.bfloat16),
            pltpu.VMEM((entries * BLOCK_ROWS, 2 * HEAD_SIZE), jnp.bfloat16),
            pltpu.VMEM((2 * BLOCK_ROWS, BLOCK_ROWS), jnp.float32),
            pltpu.VMEM((1, 128), jnp.int32),
            pltpu.VMEM((ns, 1, 128), jnp.int32),
            pltpu.SMEM((ns, 1, 128), jnp.int32),
            dma((groups, 2, nh - 1)), dma((groups, 2, nh - 1)),
            dma((groups, nh - 1)), dma((groups, nh - 1)),
            dma((groups, 3, steps)), dma((groups, 3, steps)),
            dma((groups, 3, steps)), dma((groups, 3, steps)),
            dma((groups, 3, 2 * zsz)), dma((groups, 3, 2 * zsz)),
            dma((groups, nh - 1)), dma((groups, nh - 1)),
            dma((ns - 1,)), dma((ns - 1,)),
            dma,
        ] + [pltpu.VMEM((ns * nh, 2, BLOCK_ROWS, HEAD_SIZE), jnp.bfloat16)] * groups,
        compiler_params=pltpu.CompilerParams(
            collective_id=0, has_side_effects=True, vmem_limit_bytes=60 * 1024 * 1024),
        name="block_attention",
    )(queries, keys, values, selected, counts, block_slot)


def solution(mesh):
    return jax.shard_map(
        body,
        mesh=mesh,
        in_specs=(
            P(("seq", "head"), None),
            P(("seq", "head"), None),
            P(("seq", "head"), None),
            P("seq", None),
            P("seq"),
            P("seq"),
        ),
        out_specs=P(("seq", "head"), None),
        check_vma=False,
    )
```

```python
import functools
import math

import jax
import jax.numpy as jnp
from jax import lax
from jax.experimental import pallas as pl
from jax.experimental.pallas import tpu as pltpu
from jax.sharding import PartitionSpec as P

QUERY_HEADS = 64
KEY_VALUE_HEADS = 8
HEAD_SIZE = 128
BLOCK_ROWS = 128
MESH = pl.DeviceIdType.MESH


def kernel(ns, nh, groups, entries, q_ref, k_ref, v_ref, sel_ref, cnt_ref, own_slot_ref, out_ref,
           qbuf, obuf, kcat, vcat, diag, slot_ref, slots_v, slots_s,
           hs, hr, qs, qr, us, ur, ds_, dr, ys, yr, os_, or_, ss, sr, slot_sem, *kv):
    s = lax.axis_index("seq")
    h = lax.axis_index("head")
    ysz = 2 if ns % 2 == 0 else 1
    zsz = ns // ysz
    z = s // ysz
    y = s % ysz
    y_peer = s + 1 - 2 * y
    width = qbuf.shape[3]
    heads_per_group = width // HEAD_SIZE
    rotation = [nh // 2] + [d for d in range(nh - 1, 0, -1) if d != nh // 2]

    def remote(src, dst, send, recv, dev):
        return pltpu.make_async_remote_copy(
            src_ref=src, dst_ref=dst, send_sem=send, recv_sem=recv,
            device_id=dev, device_id_type=MESH)

    lane = lax.broadcasted_iota(jnp.int32, (1, 128), 1)
    slot_row = jnp.zeros((1, 128), jnp.int32)
    for i in range(sel_ref.shape[0]):
        slot_row = jnp.where(lane == i, own_slot_ref[i], slot_row)
    slot_ref[...] = slot_row

    barrier = pltpu.get_barrier_semaphore()
    for d in range(1, nh):
        pl.semaphore_signal(barrier, inc=1, device_id=(s, (h + d) % nh), device_id_type=MESH)
    for d in range(1, ns):
        pl.semaphore_signal(barrier, inc=1, device_id=((s + d) % ns, h), device_id_type=MESH)
    pl.semaphore_wait(barrier, nh - 1 + ns - 1)

    def lanes(unit, size):
        return pl.ds(pl.multiple_of(unit * size, size), size)

    def kv_head(g, t, d):
        peer = (h + d) % nh
        src = (k_ref, v_ref)[t]
        return remote(src.at[:, lanes(peer * groups + g, HEAD_SIZE)], kv[g].at[s * nh + h, t],
                      hs.at[g, t, d - 1], hr.at[g, t, d - 1], (s, peer))

    def kv_head_in(g, t, d):
        peer = (h + nh - d) % nh
        src = (k_ref, v_ref)[t]
        return remote(src.at[:, lanes(peer * groups + g, HEAD_SIZE)], kv[g].at[s * nh + peer, t],
                      hs.at[g, t, d - 1], hr.at[g, t, d - 1], (s, peer))

    def q_head(g, d):
        peer = (h + d) % nh
        return remote(q_ref.at[:, lanes(peer * groups + g, width)], qbuf.at[g, h],
                      qs.at[g, d - 1], qr.at[g, d - 1], (s, peer))

    def q_head_in(g, d):
        peer = (h + nh - d) % nh
        return remote(q_ref.at[:, lanes(peer * groups + g, width)], qbuf.at[g, peer],
                      qs.at[g, d - 1], qr.at[g, d - 1], (s, peer))

    def slot_out(d):
        return remote(slot_ref, slots_v.at[s], ss.at[d - 1], sr.at[d - 1], ((s + d) % ns, h))

    def slot_in(d):
        peer = (s + ns - d) % ns
        return remote(slot_ref, slots_v.at[peer], ss.at[d - 1], sr.at[d - 1], (peer, h))

    for g in range(groups):
        for d in rotation:
            for t in range(2):
                kv_head(g, t, d).start()
    for d in range(1, ns):
        slot_out(d).start()
    for g in range(groups):
        for d in rotation:
            q_head(g, d).start()

    for g in range(groups):
        kv[g][s * nh + h, 0] = k_ref[:, lanes(h * groups + g, HEAD_SIZE)]
        kv[g][s * nh + h, 1] = v_ref[:, lanes(h * groups + g, HEAD_SIZE)]
        qbuf[g, h] = q_ref[:, lanes(h * groups + g, width)]
    slots_v[s] = slot_ref[...]
    pair_rows = 2 * BLOCK_ROWS
    row = lax.rem(lax.broadcasted_iota(jnp.int32, (pair_rows, BLOCK_ROWS), 0), BLOCK_ROWS)
    col = lax.broadcasted_iota(jnp.int32, (pair_rows, BLOCK_ROWS), 1)
    diag[...] = jnp.where(col <= row, 0.0, -jnp.inf).astype(jnp.float32)
    vcat[:, HEAD_SIZE:] = jnp.ones((entries * BLOCK_ROWS, HEAD_SIZE), jnp.bfloat16)

    half = nh // 2

    def early(g):
        return ysz > 1 and nh > 2 and g == groups - 1

    def part(g, shard, piece):
        lo, size = ((0, half), (half, nh - half), (nh - 1, 1))[piece]
        return kv[g].at[pl.ds(shard * nh + lo, size)]

    def cross_part(g, shard, piece):
        if piece == 1 and early(g):
            return kv[g].at[pl.ds(shard * nh + half, nh - 1 - half)]
        return part(g, shard, piece)

    def up(g, p, t, shard, dev):
        ref = part(g, shard, p)
        return remote(ref, ref, us.at[g, p, t], ur.at[g, p, t], (dev, h))

    def down(g, p, t, shard, dev):
        ref = part(g, shard, p)
        return remote(ref, ref, ds_.at[g, p, t], dr.at[g, p, t], (dev, h))

    def across(g, p, i, shard):
        ref = cross_part(g, shard, p)
        return remote(ref, ref, ys.at[g, p, i], yr.at[g, p, i], (y_peer, h))

    def pieces(g):
        return (0, 1, 2) if early(g) else (0, 1)

    def column(p):
        return y_peer if p == 2 else s

    def send_both(g, p):
        if zsz > 1:
            @pl.when(z < zsz - 1)
            def _():
                up(g, p, 0, column(p), s + ysz).start()

            @pl.when(z > 0)
            def _():
                down(g, p, 0, column(p), s - ysz).start()

    def gather_z(g):
        for d in rotation:
            for t in range(2):
                kv_head_in(g, t, d).wait_recv()
        if early(g):
            across(g, 2, 0, s).start()
        send_both(g, 0)
        send_both(g, 1)

    def gather_y(g):
        if ysz > 1:
            across(g, 0, 0, s).start()
            across(g, 1, 0, s).start()
        if early(g):
            across(g, 2, 0, y_peer).wait_recv()
            send_both(g, 2)

    def gather_step(g, t):
        for p in pieces(g):
            below = column(p) - (1 + t) * ysz
            above = column(p) + (1 + t) * ysz

            @pl.when(z - 1 - t >= 0)
            def _():
                up(g, p, t, below, s).wait_recv()
                if t + 1 < zsz - 1:
                    @pl.when(z < zsz - 1)
                    def _():
                        up(g, p, t + 1, below, s + ysz).start()
                if ysz > 1 and p < 2:
                    across(g, p, 1 + t, below).start()

            @pl.when(z + 1 + t <= zsz - 1)
            def _():
                down(g, p, t, above, s).wait_recv()
                if t + 1 < zsz - 1:
                    @pl.when(z > 0)
                    def _():
                        down(g, p, t + 1, above, s - ysz).start()
                if ysz > 1 and p < 2:
                    across(g, p, zsz + t, above).start()

    def gather_end(g):
        if ysz > 1:
            for p in range(2):
                across(g, p, 0, y_peer).wait_recv()
            for t in range(zsz - 1):
                for p in range(2):
                    @pl.when(z - 1 - t >= 0)
                    def _():
                        across(g, p, 1 + t, y_peer - (1 + t) * ysz).wait_recv()

                    @pl.when(z + 1 + t <= zsz - 1)
                    def _():
                        across(g, p, zsz + t, y_peer + (1 + t) * ysz).wait_recv()

    def gather_drain(g):
        for p in pieces(g):
            if ysz > 1:
                across(g, p, 0, s).wait_send()
            for t in range(zsz - 1):
                @pl.when((z < zsz - 1) & (z - t >= 0))
                def _():
                    up(g, p, t, column(p) - t * ysz, s + ysz).wait_send()

                @pl.when((z > 0) & (z + t <= zsz - 1))
                def _():
                    down(g, p, t, column(p) + t * ysz, s - ysz).wait_send()
                if ysz > 1 and p < 2:
                    @pl.when(z - 1 - t >= 0)
                    def _():
                        across(g, p, 1 + t, s - (1 + t) * ysz).wait_send()

                    @pl.when(z + 1 + t <= zsz - 1)
                    def _():
                        across(g, p, zsz + t, s + (1 + t) * ysz).wait_send()

    factor = math.log2(math.e) / math.sqrt(HEAD_SIZE)
    blk_seq = sel_ref.shape[0]

    def fetch(g, j):
        for e in range(entries):
            b = sel_ref[j, e]
            place = slots_s[lax.div(b, blk_seq), 0, lax.rem(b, blk_seq)]
            rows = slice(e * BLOCK_ROWS, (e + 1) * BLOCK_ROWS)
            kcat[rows, :] = kv[g][place, 0]
            vcat[rows, :HEAD_SIZE] = kv[g][place, 1]

    def attend(g, j):
        rest = lax.broadcasted_iota(jnp.int32, (1, (entries - 1) * BLOCK_ROWS), 1) + BLOCK_ROWS
        bias = jnp.where(rest < cnt_ref[j] * BLOCK_ROWS, 0.0, -jnp.inf).astype(jnp.float32)

        def pair(i, _):
            cols = pl.multiple_of(i * 2 * HEAD_SIZE, 2 * HEAD_SIZE)
            q2 = qbuf[g, j, :, pl.ds(cols, 2 * HEAD_SIZE)]
            q2 = jnp.concatenate([q2[:, :HEAD_SIZE], q2[:, HEAD_SIZE:]], axis=0)
            scores = lax.dot_general(q2, kcat[...], (((1,), (1,)), ((), ())),
                                     preferred_element_type=jnp.float32)
            own = scores[:, :BLOCK_ROWS] + diag[...]
            others = scores[:, BLOCK_ROWS:] + bias
            scores = jnp.concatenate([own, others], axis=1)
            top = jnp.max(scores, axis=1, keepdims=True)
            weights = jnp.exp2((scores - top) * factor).astype(jnp.bfloat16)
            mixed = jnp.dot(weights, vcat[...], preferred_element_type=jnp.float32)
            result = (mixed[:, :HEAD_SIZE] / mixed[:, HEAD_SIZE:]).astype(jnp.bfloat16)
            obuf[g, j, :, pl.ds(cols, HEAD_SIZE)] = result[:BLOCK_ROWS]
            obuf[g, j, :, pl.ds(cols + HEAD_SIZE, HEAD_SIZE)] = result[BLOCK_ROWS:]
            return 0

        lax.fori_loop(0, heads_per_group // 2, pair, 0, unroll=True)

    def result_out(g, d):
        peer = (h + d) % nh
        return remote(obuf.at[g, peer], out_ref.at[:, lanes(h * groups + g, width)],
                      os_.at[g, d - 1], or_.at[g, d - 1], (s, peer))

    def result_in(g, d):
        peer = (h + nh - d) % nh
        return remote(obuf.at[g, peer], out_ref.at[:, lanes(peer * groups + g, width)],
                      os_.at[g, d - 1], or_.at[g, d - 1], (s, peer))

    def slot_table():
        for d in range(1, ns):
            slot_in(d).wait_recv()
        slot_copy = pltpu.make_async_copy(slots_v, slots_s, slot_sem)
        slot_copy.start()
        slot_copy.wait()

    if nh == 4:
        order = [2, 3 - 2 * (h % 2), 1 + 2 * (h % 2), 0]
    else:
        order = rotation + [0]
    gather_z(0)
    gather_y(0)
    for t in range(zsz - 2):
        gather_step(0, t)
    pending = None
    for g in range(groups):
        more = g + 1 < groups
        if more:
            gather_z(g + 1)
        if g == 0 and zsz > 1:
            gather_step(0, zsz - 2)
        steps = []
        if more:
            gather_y(g + 1)
            steps = list(range(zsz - 1))
            if steps:
                gather_step(g + 1, steps.pop(0))
        if g == 0:
            slot_table()
        gather_end(g)
        for n, d in enumerate(order):
            own = n == len(order) - 1
            j = (h + d) % nh
            fetch(g, j)
            if pending is not None:
                result_out(*pending).start()
                pending = None
            if not own:
                q_head_in(g, nh - d).wait_recv()
            if n >= len(order) // 2 and len(steps) > 1:
                gather_step(g + 1, steps.pop(0))
            attend(g, j)
            if own:
                out_ref[:, lanes(h * groups + g, width)] = obuf[g, h]
            else:
                pending = (g, d)
        for t in steps:
            gather_step(g + 1, t)

    for g in range(groups):
        gather_drain(g)
        for d in rotation:
            for t in range(2):
                kv_head(g, t, d).wait_send()
            q_head(g, d).wait_send()
    for d in range(1, ns):
        slot_out(d).wait_send()
    for g in range(groups):
        for d in rotation:
            result_out(g, d).wait_send()
            result_in(g, d).wait_recv()


def body(queries, keys, values, selected, counts, block_slot):
    ns = lax.axis_size("seq")
    nh = lax.axis_size("head")
    blk_seq, entries = selected.shape
    rows = queries.shape[0]
    groups = keys.shape[1] // HEAD_SIZE // nh
    width = queries.shape[1] // nh // groups
    assert rows == BLOCK_ROWS and blk_seq == nh
    vmem = pl.BlockSpec(memory_space=pltpu.VMEM)
    smem = pl.BlockSpec(memory_space=pltpu.SMEM)
    zsz = ns // (2 if ns % 2 == 0 else 1)
    dma = pltpu.SemaphoreType.DMA
    steps = max(zsz - 1, 1)
    return pl.pallas_call(
        functools.partial(kernel, ns, nh, groups, entries),
        out_shape=jax.ShapeDtypeStruct(queries.shape, jnp.bfloat16),
        in_specs=[vmem, vmem, vmem, smem, smem, smem],
        out_specs=vmem,
        scratch_shapes=[
            pltpu.VMEM((groups, nh, rows, width), jnp.bfloat16),
            pltpu.VMEM((groups, nh, rows, width), jnp.bfloat16),
            pltpu.VMEM((entries * BLOCK_ROWS, HEAD_SIZE), jnp.bfloat16),
            pltpu.VMEM((entries * BLOCK_ROWS, 2 * HEAD_SIZE), jnp.bfloat16),
            pltpu.VMEM((2 * BLOCK_ROWS, BLOCK_ROWS), jnp.float32),
            pltpu.VMEM((1, 128), jnp.int32),
            pltpu.VMEM((ns, 1, 128), jnp.int32),
            pltpu.SMEM((ns, 1, 128), jnp.int32),
            dma((groups, 2, nh - 1)), dma((groups, 2, nh - 1)),
            dma((groups, nh - 1)), dma((groups, nh - 1)),
            dma((groups, 3, steps)), dma((groups, 3, steps)),
            dma((groups, 3, steps)), dma((groups, 3, steps)),
            dma((groups, 3, 2 * zsz)), dma((groups, 3, 2 * zsz)),
            dma((groups, nh - 1)), dma((groups, nh - 1)),
            dma((ns - 1,)), dma((ns - 1,)),
            dma,
        ] + [pltpu.VMEM((ns * nh, 2, BLOCK_ROWS, HEAD_SIZE), jnp.bfloat16)] * groups,
        compiler_params=pltpu.CompilerParams(
            collective_id=0, has_side_effects=True, vmem_limit_bytes=60 * 1024 * 1024),
        name="block_attention",
    )(queries, keys, values, selected, counts, block_slot)


def solution(mesh):
    return jax.shard_map(
        body,
        mesh=mesh,
        in_specs=(
            P(("seq", "head"), None),
            P(("seq", "head"), None),
            P(("seq", "head"), None),
            P("seq", None),
            P("seq"),
            P("seq"),
        ),
        out_specs=P(("seq", "head"), None),
        check_vma=False,
    )
```
